256 devices in a mesh: gx: 8 (over y, core), gy: 32 (over z, x).
Axes of the slice: x: 4, y: 4, z: 8, core: 2. Of those that a mesh axis runs over, the one named last changes fastest.
Arguments:
- tokens: bfloat16 [1024, 4096], P('gy', 'gx'), may hold values from -140 to 140
- cotangent: bfloat16 [1024, 4096], P('gy', 'gx'), may hold values from -6 to 6
- gate_weight: bfloat16 [4096, 14336], P('gx', 'gy'), may hold values from -5 to 5
- up_weight: bfloat16 [4096, 14336], P('gx', 'gy'), may hold values from -5 to 5
- down_weight: bfloat16 [14336, 4096], P('gy', 'gx'), may hold values from -5 to 5
Outputs:
- output: bfloat16 [1024, 4096], P('gy', 'gx')
- input_grad: bfloat16 [1024, 4096], P('gy', 'gx')
- gate_grad: bfloat16 [4096, 14336], P('gx', 'gy')
- up_grad: bfloat16 [4096, 14336], P('gx', 'gy')
- down_grad: bfloat16 [14336, 4096], P('gy', 'gx')
The draws below stay inside these ranges and needn't reach their ends.
All inputs are finite; a program needn't handle non-finite values.
Results may differ from the reference program's by a relative error of at most 0.005.
The reference program's roundings to bfloat16 on the way count: a program that leaves them out, or rounds other values in their place, can miss the bound.
Values may be sent and summed in bfloat16 or wider, within the bound.
No kernel may reach another device: no remote copies, remote signals or barrier semaphores. Data moves between devices by JAX's collectives and lax.ppermute only.
A program may use at most 64 MiB of HBM per device.

```python
import jax
import jax.numpy as jnp
from jax import lax

D = 4096
FF = 14336
ROT_BLOCK = 128
HID_BLOCK = 64
TOKENS = 1024


def rising_weight(key, row_total, col_total, fan_in):
    key_base, key_cols = jax.random.split(key)
    base = jnp.clip(jax.random.normal(key_base, (row_total, col_total), jnp.float32), -4.0, 4.0)
    row_frac = jnp.arange(row_total, dtype=jnp.float32)[:, None] / max(row_total - 1, 1)
    col_frac = jnp.arange(col_total, dtype=jnp.float32)[None, :] / max(col_total - 1, 1)
    col_rough = jnp.exp(jax.random.uniform(key_cols, (1, col_total), jnp.float32, 0.0, jnp.log(3.0)))
    rise = jnp.exp(jnp.log(3.0) * (row_frac + col_frac)) * col_rough
    return base * rise / (3.0 * fan_in ** 0.5)


def draw_tokens(key, part):
    key_base, key_rows, key_cols = jax.random.split(jax.random.fold_in(key, 11), 3)
    base = jnp.clip(jax.random.normal(key_base, (TOKENS, D), jnp.float32), -4.0, 4.0)
    row_rough = jnp.exp(jax.random.uniform(key_rows, (TOKENS, 1), jnp.float32, 0.0, jnp.log(3.3)))
    col_rough = jnp.exp(jax.random.uniform(key_cols, (1, D), jnp.float32, 0.0, jnp.log(3.0)))
    row_frac = jnp.arange(TOKENS, dtype=jnp.float32)[:, None] / max(TOKENS - 1, 1)
    col_frac = jnp.arange(D, dtype=jnp.float32)[None, :] / max(D - 1, 1)
    rise = jnp.exp(jnp.log(3.0) * (row_frac + col_frac))
    return (base * rise * row_rough * col_rough / 8.0).astype(jnp.bfloat16)


def draw_gate_weight(key, part):
    return rising_weight(jax.random.fold_in(key, 21), D, FF, D).astype(jnp.bfloat16)


def draw_up_weight(key, part):
    return rising_weight(jax.random.fold_in(key, 31), D, FF, D).astype(jnp.bfloat16)


def draw_down_weight(key, part):
    return rising_weight(jax.random.fold_in(key, 41), FF, D, FF).astype(jnp.bfloat16)


def block_levels(rng, extent, cuts, least, largest):
    loudness = 1.0
    for dim, parts in cuts:
        draws = jax.random.uniform(jax.random.fold_in(jax.random.fold_in(rng, 6), dim), (parts,), jnp.float32, least / len(cuts), largest / len(cuts))
        loudness = loudness * jnp.repeat(jnp.exp(draws), extent[dim] // parts).reshape((-1,) + (1,) * (len(extent) - 1 - dim))
    return loudness


def gaussian(own_key, shape, spread, most, cuts=(), kind=jnp.bfloat16):
    factor_of = block_levels(own_key, shape, cuts, -0.22, 0.18) if cuts else 1.0
    array = jax.random.normal(own_key, shape, jnp.float32) * spread * factor_of
    return jnp.minimum(jnp.maximum(array, -most), most).astype(kind)


def setup_inputs(seed: int = 0) -> dict:
    keys = jax.random.split(jax.random.key(seed), 6)
    return {
        "tokens": draw_tokens(jax.random.fold_in(keys[5], 71), 0),
        "cotangent": gaussian(keys[1], (TOKENS, D), 1.0, 6.0, ((0, 32), (1, 8))),
        "gate_weight": draw_gate_weight(jax.random.fold_in(keys[5], 71), 0),
        "up_weight": draw_up_weight(jax.random.fold_in(keys[5], 71), 0),
        "down_weight": draw_down_weight(jax.random.fold_in(keys[5], 71), 0),
    }


fp_top = 448.0
tiny = 1e-6


def hadamard_table(block_size):
    row_ids = jnp.arange(block_size, dtype=jnp.int32)[:, None]
    col_ids = jnp.arange(block_size, dtype=jnp.int32)[None, :]
    shared = row_ids & col_ids
    parity = jnp.zeros((block_size, block_size), jnp.int32)
    for bit_pos in range(max(block_size.bit_length() - 1, 1)):
        parity = parity + ((shared >> bit_pos) & 1)
    return (1 - 2 * (parity % 2)).astype(jnp.float32)


def rotate_cols(matrix, block_size):
    row_total, col_total = matrix.shape
    table = hadamard_table(block_size)
    blocks = matrix.astype(jnp.float32).reshape(row_total, col_total // block_size, block_size)
    turned = jnp.einsum("rbk,kl->rbl", blocks, table, precision=lax.Precision.HIGHEST)
    return turned.reshape(row_total, col_total) * (block_size ** -0.5)


def rotate_rows(matrix, block_size):
    row_total, col_total = matrix.shape
    table = hadamard_table(block_size)
    blocks = matrix.astype(jnp.float32).reshape(row_total // block_size, block_size, col_total)
    turned = jnp.einsum("kl,bkc->blc", table, blocks, precision=lax.Precision.HIGHEST)
    return turned.reshape(row_total, col_total) * (block_size ** -0.5)


def soft_cast(values, top):
    return (fp_top * jnp.tanh(values / (top + tiny))).astype(jnp.bfloat16)


def peak(values):
    return jnp.max(jnp.abs(values))


def reference(tokens, cotangent, gate_weight, up_weight, down_weight):
    token_rot = rotate_cols(tokens, ROT_BLOCK)
    gate_rot = rotate_rows(gate_weight, ROT_BLOCK)
    up_rot = rotate_rows(up_weight, ROT_BLOCK)
    down_rot = rotate_rows(down_weight, HID_BLOCK)
    token_peak = peak(token_rot)
    gate_peak = peak(gate_rot)
    up_peak = peak(up_rot)
    down_peak = peak(down_rot)
    token_cast = soft_cast(token_rot, token_peak)
    gate_cast = soft_cast(gate_rot, gate_peak)
    up_cast = soft_cast(up_rot, up_peak)
    down_cast = soft_cast(down_rot, down_peak)
    gate_pre = jnp.dot(token_cast, gate_cast, preferred_element_type=jnp.float32) * (token_peak * gate_peak / (fp_top * fp_top))
    up_pre = jnp.dot(token_cast, up_cast, preferred_element_type=jnp.float32) * (token_peak * up_peak / (fp_top * fp_top))
    hidden = (jax.nn.silu(gate_pre) * up_pre).astype(jnp.bfloat16)
    hidden_rot = rotate_cols(hidden, HID_BLOCK)
    hidden_peak = peak(hidden_rot)
    hidden_cast = soft_cast(hidden_rot, hidden_peak)
    output = (jnp.dot(hidden_cast, down_cast, preferred_element_type=jnp.float32) * (hidden_peak * down_peak / (fp_top * fp_top))).astype(jnp.bfloat16)
    down_grad = rotate_rows(jnp.dot(hidden_cast.T, cotangent, preferred_element_type=jnp.float32) * (hidden_peak / fp_top), HID_BLOCK).astype(jnp.bfloat16)
    hidden_grad = rotate_cols(jnp.dot(cotangent, down_cast.T, preferred_element_type=jnp.float32) * (down_peak / fp_top), HID_BLOCK)
    sigmoid_gate = jax.nn.sigmoid(gate_pre)
    gate_act = (hidden_grad * up_pre * sigmoid_gate * (1.0 + gate_pre * (1.0 - sigmoid_gate))).astype(jnp.bfloat16)
    up_act = (hidden_grad * gate_pre * sigmoid_gate).astype(jnp.bfloat16)
    gate_grad = rotate_rows(jnp.dot(token_cast.T, gate_act, preferred_element_type=jnp.float32) * (token_peak / fp_top), ROT_BLOCK).astype(jnp.bfloat16)
    up_grad = rotate_rows(jnp.dot(token_cast.T, up_act, preferred_element_type=jnp.float32) * (token_peak / fp_top), ROT_BLOCK).astype(jnp.bfloat16)
    input_sum = jnp.dot(gate_act, gate_cast.T, preferred_element_type=jnp.float32) * (gate_peak / fp_top) + jnp.dot(up_act, up_cast.T, preferred_element_type=jnp.float32) * (up_peak / fp_top)
    input_grad = rotate_cols(input_sum, ROT_BLOCK).astype(jnp.bfloat16)
    return (output, input_grad, gate_grad, up_grad, down_grad)
```

```python
import jax
import jax.numpy as jnp
from jax import lax
from jax.experimental.layout import Layout, with_layout_constraint
from jax.sharding import Mesh
from jax.sharding import PartitionSpec as P


ROT_BLOCK = 128
HID_BLOCK = 64
NY, NC, NZ, NX = 4, 2, 8, 4
GX = ("y", "c")
GY = ("z", "x")
ALL = ("y", "c", "z", "x")


fp_top = 448.0
tiny = 1e-06
bf16 = jnp.bfloat16
f16 = jnp.float16
f32 = jnp.float32


def hadamard_table(block_size):
    row_ids = jnp.arange(block_size, dtype=jnp.int32)[:, None]
    col_ids = jnp.arange(block_size, dtype=jnp.int32)[None, :]
    shared = row_ids & col_ids
    parity = jnp.zeros((block_size, block_size), jnp.int32)
    for bit_pos in range(max(block_size.bit_length() - 1, 1)):
        parity = parity + (shared >> bit_pos & 1)
    return (1 - 2 * (parity % 2)).astype(f32)


def rotate_cols(matrix, block_size):
    row_total, col_total = matrix.shape
    table = hadamard_table(block_size)
    blocks = matrix.reshape(row_total, col_total // block_size, block_size)
    if matrix.dtype == bf16:
        turned = jnp.einsum("rbk,kl->rbl", blocks, table.astype(bf16), preferred_element_type=f32)
    else:
        turned = jnp.einsum("rbk,kl->rbl", blocks, table, precision=lax.Precision.HIGHEST)
    return turned.reshape(row_total, col_total) * block_size ** (-0.5)


def rotate_rows(matrix, block_size):
    row_total, col_total = matrix.shape
    table = hadamard_table(block_size)
    blocks = matrix.reshape(row_total // block_size, block_size, col_total)
    if matrix.dtype == bf16:
        turned = jnp.einsum("kl,bkc->blc", table.astype(bf16), blocks, preferred_element_type=f32)
    else:
        turned = jnp.einsum("kl,bkc->blc", table, blocks, precision=lax.Precision.HIGHEST)
    return turned.reshape(row_total, col_total) * block_size ** (-0.5)


def soft_cast(values, top):
    return (fp_top * jnp.tanh(values / (top + tiny))).astype(bf16)


def peak(values):
    return jnp.max(jnp.abs(values))


def dot(left, right, left_dim, right_dim):
    return lax.dot_general(
        left, right, (((left_dim,), (right_dim,)), ((), ())), preferred_element_type=f32
    )


def everyones(values):
    copies = jnp.broadcast_to(values, (NY * NC * NZ * NX, 1, values.shape[0]))
    return lax.all_to_all(copies, ALL, 0, 0, tiled=True).max(axis=(0, 1))


def swapped(value):
    return lax.ppermute(value, "c", [(0, 1), (1, 0)])


def shifted(value, axis, size, step):
    return lax.ppermute(value, axis, [(i, (i + step) % size) for i in range(size)])


def along_x(value, step, back=False):
    pairs = []
    for c in range(NC):
        for x in range(NX):
            to = c * NX + (x + (step if c == 0 else -step)) % NX
            pairs.append((to, c * NX + x) if back else (c * NX + x, to))
    return lax.ppermute(value, ("c", "x"), pairs)


def copied(value, axes, count):
    return lax.all_to_all(jnp.broadcast_to(value, (count, *value.shape)), axes, 0, 0, tiled=True)


def halves_along_x(column, first):
    far = shifted(column, "x", NX, 2)
    near, last = along_x(column, 1), along_x(column, 3)
    mine = jnp.concatenate([jnp.where(first, column, far), near], axis=0)
    other = jnp.concatenate([jnp.where(first, far, column), last], axis=0)
    return mine, other


def scatter_tokens(mine, other, first, kind):
    rows, width = mine.shape[0] // 2, mine.shape[1]
    m, o = mine.reshape(2, rows, width), other.reshape(2, rows, width)
    near = along_x(m[1].astype(kind), 1, back=True)
    last = along_x(o[1].astype(kind), 3, back=True)
    far = shifted(jnp.where(first, o[0], m[0]).astype(kind), "x", NX, 2)
    column = jnp.where(first, m[0], o[0]) + near.astype(f32) + last.astype(f32) + far.astype(f32)
    pieces = column.astype(kind).reshape(NZ, rows // NZ, width)
    return lax.all_to_all(pieces, "z", 0, 0, tiled=True).astype(f32).sum(axis=0)


def scatter_width(mine, theirs, kind, scale):
    both = mine * scale + swapped((theirs * scale).astype(kind)).astype(f32)
    blocks = both.reshape(NY, both.shape[0] // NY, both.shape[1])
    me = lax.axis_index("y")
    total = lax.dynamic_index_in_dim(blocks, me, 0, keepdims=False)
    for step in range(1, NY):
        sent = lax.dynamic_index_in_dim(blocks, (me + step) % NY, 0, keepdims=False)
        total = total + shifted(sent.astype(kind), "y", NY, step).astype(f32)
    return total


def gather_half(value):
    value = row_major(value)
    me = lax.axis_index("y")
    out = jnp.zeros((NY, *value.shape), value.dtype)
    out = lax.dynamic_update_index_in_dim(out, value, me, 0)
    for step in range(1, NY):
        got = shifted(value, "y", NY, step)
        out = lax.dynamic_update_index_in_dim(out, got, (me - step) % NY, 0)
    return row_major(out).reshape(NY * value.shape[0], value.shape[1])


def row_major(array):
    return with_layout_constraint(array, Layout(major_to_minor=tuple(range(array.ndim))))


def padded(array, dim):
    extra = -array.shape[dim] % 128
    widths = [(0, extra if d == dim else 0) for d in range(array.ndim)]
    return jnp.pad(array, widths)


def column_peaks(values):
    return padded(jnp.max(jnp.abs(values), axis=0, keepdims=True), 1)


def greatest(tops, after):
    other = swapped(tops)
    tops = jnp.maximum(tops, other)
    for axis, size in (("y", NY), ("x", NX)):
        got = [shifted(tops, axis, size, step) for step in range(1, size)]
        for g in got:
            tops = jnp.maximum(tops, g)
    tops, _ = lax.optimization_barrier((tops, after))
    return copied(tops, "z", NZ).max(axis=(0, 2))


def layer(tokens, cotangent, gate_weight, up_weight, down_weight):
    hid = gate_weight.shape[1]
    rows = tokens.shape[0]
    first = lax.axis_index("c") == 0

    column = copied(jnp.concatenate([tokens, cotangent], axis=0), "z", NZ)
    token_column = column[:, :rows].reshape(NZ * rows, tokens.shape[1])
    cot_column = column[:, rows:].reshape(NZ * rows, tokens.shape[1])

    gate_rot = rotate_rows(gate_weight, ROT_BLOCK)
    up_rot = rotate_rows(up_weight, ROT_BLOCK)
    down_rot = rotate_rows(down_weight, HID_BLOCK)
    token_rot = rotate_cols(tokens, ROT_BLOCK)
    peaks = greatest(
        jnp.concatenate([column_peaks(v) for v in (gate_rot, up_rot, down_rot, token_rot)], axis=0),
        column,
    )
    gate_peak, up_peak, down_peak, token_peak = peaks[0], peaks[1], peaks[2], peaks[3]
    gate_cast = padded(soft_cast(gate_rot, gate_peak), 1)
    up_cast = padded(soft_cast(up_rot, up_peak), 1)
    down_cast = padded(soft_cast(down_rot, down_peak), 0)
    wide = gate_cast.shape[1]
    weight_pair = jnp.concatenate([gate_cast, up_cast], axis=1)

    mine_tokens, their_tokens = halves_along_x(token_column, first)
    mine_cot, their_cot = halves_along_x(cot_column, first)

    their_tok = soft_cast(rotate_cols(their_tokens, ROT_BLOCK), token_peak)
    mine_tok = soft_cast(rotate_cols(mine_tokens, ROT_BLOCK), token_peak)
    paired = scatter_width(
        dot(mine_tok, weight_pair, 1, 0), dot(their_tok, weight_pair, 1, 0), f16, 2.0**-12
    )
    gate_pre = paired[:, :wide] * (token_peak * gate_peak / (fp_top * fp_top) * 2.0**12)
    up_pre = paired[:, wide:] * (token_peak * up_peak / (fp_top * fp_top) * 2.0**12)

    hidden = (jax.nn.silu(gate_pre) * up_pre).astype(bf16)
    hidden_peak = everyones(peak(rotate_cols(hidden, HID_BLOCK))[None])[0]
    mine_hid = gather_half(hidden)
    their_hid = swapped(mine_hid)

    back_sum = scatter_width(
        dot(mine_cot, down_cast, 1, 1), dot(their_cot, down_cast, 1, 1), f16, 2.0**-6
    )
    hidden_grad = rotate_cols(back_sum * (down_peak / fp_top * 2.0**6), HID_BLOCK)
    sigmoid_gate = jax.nn.sigmoid(gate_pre)
    gate_act = (
        hidden_grad * up_pre * sigmoid_gate * (1.0 + gate_pre * (1.0 - sigmoid_gate))
    ).astype(bf16)
    up_act = (hidden_grad * gate_pre * sigmoid_gate).astype(bf16)
    mine_act = gather_half(jnp.concatenate([gate_act, up_act], axis=1))
    their_act = swapped(mine_act)

    def out_part(half):
        cast = soft_cast(rotate_cols(half, HID_BLOCK), hidden_peak)
        return cast, dot(cast, down_cast, 1, 0) * 2.0**-13

    (mine_hid_cast, mine_out), (their_hid_cast, their_out) = out_part(mine_hid), out_part(their_hid)
    out_sum = scatter_tokens(mine_out, their_out, first, f16)
    output = (out_sum * (hidden_peak * down_peak / (fp_top * fp_top) * 2.0**13)).astype(bf16)

    def in_part(half):
        return dot(half[:, :wide], gate_cast, 1, 1) * (gate_peak / fp_top) + dot(
            half[:, wide:], up_cast, 1, 1
        ) * (up_peak / fp_top)

    input_sum = scatter_tokens(in_part(mine_act), in_part(their_act), first, bf16)
    input_grad = rotate_cols(input_sum, ROT_BLOCK).astype(bf16)

    down_dot = dot(mine_hid_cast, mine_cot, 0, 0) + dot(their_hid_cast, their_cot, 0, 0)
    down_grad = rotate_rows(down_dot[:hid] * (hidden_peak / fp_top), HID_BLOCK)
    pair_dot = dot(mine_tok, mine_act, 0, 0) + dot(their_tok, their_act, 0, 0)
    pair_grad = rotate_rows(pair_dot * (token_peak / fp_top), ROT_BLOCK).astype(bf16)
    return (
        output,
        input_grad,
        pair_grad[:, :hid],
        pair_grad[:, wide : wide + hid],
        down_grad.astype(bf16),
    )


def solution(mesh):
    split = Mesh(mesh.devices.reshape(NY, NC, NZ, NX), ALL)
    placed = (P(GY, GX), P(GY, GX), P(GX, GY), P(GX, GY), P(GY, GX))
    return jax.shard_map(
        layer,
        mesh=split,
        in_specs=placed,
        out_specs=(P(GY, GX), P(GY, GX), P(GX, GY), P(GX, GY), P(GY, GX)),
        check_vma=False,
    )
```

```python
import jax
import jax.numpy as jnp
from jax import lax
from jax.experimental import pallas as pl
from jax.experimental.layout import Layout, with_layout_constraint
from jax.experimental.pallas import tpu as pltpu
from jax.sharding import Mesh
from jax.sharding import PartitionSpec as P


ROT_BLOCK = 128
HID_BLOCK = 64
NY, NC, NZ, NX = 4, 2, 8, 4
GX = ("y", "c")
GY = ("z", "x")
ALL = ("y", "c", "z", "x")


fp_top = 448.0
tiny = 1e-06
bf16 = jnp.bfloat16
f16 = jnp.float16
f32 = jnp.float32


def hadamard_table(block_size):
    row_ids = jnp.arange(block_size, dtype=jnp.int32)[:, None]
    col_ids = jnp.arange(block_size, dtype=jnp.int32)[None, :]
    shared = row_ids & col_ids
    parity = jnp.zeros((block_size, block_size), jnp.int32)
    for bit_pos in range(max(block_size.bit_length() - 1, 1)):
        parity = parity + (shared >> bit_pos & 1)
    return (1 - 2 * (parity % 2)).astype(f32)


def wide_table(block_size, i):
    parity = jnp.zeros((i.shape[0], i.shape[0]), jnp.int32)
    shared = i[:, None] & i[None, :]
    for bit_pos in range(block_size.bit_length() - 1):
        parity = parity + (shared >> bit_pos & 1)
    same = i[:, None] // block_size == i[None, :] // block_size
    return jnp.where(same, 1 - 2 * (parity % 2), 0).astype(bf16)


def rotate_cols(matrix, block_size, wide=None):
    row_total, col_total = matrix.shape
    table = hadamard_table(block_size)
    if wide is not None:
        turned = dot(matrix, wide, 1, 0)
    else:
        blocks = matrix.reshape(row_total, col_total // block_size, block_size)
        turned = jnp.einsum("rbk,kl->rbl", blocks, table, precision=lax.Precision.HIGHEST)
    return turned.reshape(row_total, col_total) * block_size ** (-0.5)


def rotate_rows(matrix, block_size, wide=None):
    row_total, col_total = matrix.shape
    table = hadamard_table(block_size)
    if wide is not None:
        turned = dot(wide, matrix, 1, 0)
    else:
        blocks = matrix.reshape(row_total // block_size, block_size, col_total)
        turned = jnp.einsum("kl,bkc->blc", table, blocks, precision=lax.Precision.HIGHEST)
    return turned.reshape(row_total, col_total) * block_size ** (-0.5)


def soft_cast(values, top):
    return (fp_top * jnp.tanh(values / (top + tiny))).astype(bf16)


def dot(left, right, left_dim, right_dim):
    return lax.dot_general(
        left, right, (((left_dim,), (right_dim,)), ((), ())), preferred_element_type=f32
    )


def after(values, *earlier):
    return lax.optimization_barrier((values, earlier))[0]


def swapped(value):
    return lax.ppermute(value, "c", [(0, 1), (1, 0)])


def shifted(value, axis, size, step):
    return lax.ppermute(value, axis, [(i, (i + step) % size) for i in range(size)])


def along_x(value, step, back=False):
    pairs = []
    for c in range(NC):
        for x in range(NX):
            to = c * NX + (x + (step if c == 0 else -step)) % NX
            pairs.append((to, c * NX + x) if back else (c * NX + x, to))
    return lax.ppermute(value, ("c", "x"), pairs)


def copied(value, axes, count):
    return lax.all_to_all(jnp.broadcast_to(value, (count, *value.shape)), axes, 0, 0, tiled=True)


def blocks_along_x(column):
    return column, shifted(column, "x", NX, 2), along_x(column, 1), along_x(column, 3)


def halves_along_x(blocks, first):
    column, far, near, last = blocks
    mine = jnp.concatenate([jnp.where(first, column, far), near], axis=0)
    other = jnp.concatenate([jnp.where(first, far, column), last], axis=0)
    return mine, other


def sum_along_x(mine, other, first, kind):
    rows, width = mine.shape[0] // 2, mine.shape[1]
    m, o = mine.reshape(2, rows, width), other.reshape(2, rows, width)
    sends = (
        m[1].astype(kind),
        o[1].astype(kind),
        jnp.where(first, o[0], m[0]).astype(kind),
    )
    near = along_x(sends[0], 1, back=True)
    last = along_x(sends[1], 3, back=True)
    far = shifted(sends[2], "x", NX, 2)
    column = jnp.where(first, m[0], o[0]) + near.astype(f32) + last.astype(f32) + far.astype(f32)
    return column.astype(kind), sends


def pieces_along_z(column):
    pieces = column.reshape(NZ, column.shape[0] // NZ, column.shape[1])
    return lax.all_to_all(pieces, "z", 0, 0, tiled=True)


def scatter_width(mine, theirs, kind):
    got = swapped(theirs.astype(kind))
    blocks = (mine + got.astype(f32)).reshape(NY, mine.shape[0] // NY, mine.shape[1])
    me = lax.axis_index("y")
    total = lax.dynamic_index_in_dim(blocks, me, 0, keepdims=False)
    sends = [
        lax.dynamic_index_in_dim(blocks, (me + step) % NY, 0, keepdims=False).astype(kind)
        for step in range(1, NY)
    ]
    for step in range(1, NY):
        total = total + shifted(sends[step - 1], "y", NY, step).astype(f32)
    return total


def join_kernel(me_ref, own_ref, got1_ref, got2_ref, got3_ref, out_ref):
    rows = own_ref.shape[0]
    for step, ref in enumerate((own_ref, got1_ref, got2_ref, got3_ref)):
        at = pl.multiple_of(((me_ref[0] + NY - step) & (NY - 1)) * rows, rows)
        out_ref[pl.ds(at, rows), :] = ref[...]


def gather_half(value):
    got = [shifted(value, "y", NY, step) for step in range(1, NY)]
    vmem = pl.BlockSpec(memory_space=pltpu.VMEM)
    mine = pl.pallas_call(
        join_kernel,
        out_shape=jax.ShapeDtypeStruct((NY * value.shape[0], value.shape[1]), value.dtype),
        in_specs=[pl.BlockSpec(memory_space=pltpu.SMEM)] + [vmem] * NY,
        out_specs=vmem,
        name="join",
    )(lax.axis_index("y")[None], value, *got)
    return mine, swapped(mine)


def middle_kernel(sums_ref, scales_ref, table_ref, out_ref, top_ref):
    wide = scales_ref.shape[1]
    table = table_ref[...]
    top = jnp.zeros((8, 128), f32)
    for at in range(0, wide, 128):
        gate = sums_ref[:, at : at + 128] * scales_ref[0:1, at : at + 128]
        up = sums_ref[:, wide + at : wide + at + 128] * scales_ref[1:2, at : at + 128]
        back = sums_ref[:, 2 * wide + at : 2 * wide + at + 128] * scales_ref[2:3, at : at + 128]
        sig = jax.nn.sigmoid(gate)
        hidden = (gate * sig * up).astype(bf16)
        turned = jnp.abs(jnp.dot(hidden, table, preferred_element_type=f32)) * HID_BLOCK**-0.5
        for row in range(0, turned.shape[0], 8):
            top = jnp.maximum(top, turned[row : row + 8])
        grad = jnp.zeros(back.shape, f32)
        for _ in range(3):
            term = back.astype(bf16)
            grad = grad + jnp.dot(term, table, preferred_element_type=f32)
            back = back - term.astype(f32)
        grad = grad * HID_BLOCK**-0.5
        gate_act = grad * up * sig * (1.0 + gate * (1.0 - sig))
        out_ref[:, at : at + 128] = gate_act.astype(bf16)
        out_ref[:, wide + at : wide + at + 128] = (grad * gate * sig).astype(bf16)
        out_ref[:, 2 * wide + at : 2 * wide + at + 128] = hidden
    top_ref[...] = top


def row_major(array):
    return with_layout_constraint(array, Layout(major_to_minor=tuple(range(array.ndim))))


def padded(array, dim):
    extra = -array.shape[dim] % 128
    widths = [(0, extra if d == dim else 0) for d in range(array.ndim)]
    return jnp.pad(array, widths)


def column_peaks(values):
    return jnp.max(jnp.abs(values), axis=0, keepdims=True)


def everyones(values):
    copies = jnp.broadcast_to(values, (NY * NC * NZ * NX, 1, values.shape[0]))
    return lax.all_to_all(copies, ALL, 0, 0, tiled=True).max(axis=(0, 1))


def rotate_rows_split(matrix, block_size, wide):
    total = 0.0
    for _ in range(3):
        term = lax.reduce_precision(matrix, 8, 7)
        total = total + dot(wide, term.astype(bf16), 1, 0)
        matrix = matrix - term
    return total * block_size ** (-0.5)


def layer(tokens, cotangent, gate_weight, up_weight, down_weight):
    hid = gate_weight.shape[1]
    rows, features = tokens.shape
    core = lax.axis_index("c")
    first = core == 0

    column = copied(jnp.concatenate([tokens, cotangent], axis=0), "z", NZ)
    token_column = column[:, :rows].reshape(NZ * rows, features)
    cot_column = column[:, rows:].reshape(NZ * rows, features)

    ids = lax.optimization_barrier(jnp.arange(features, dtype=jnp.int32))
    rot_wide, hid_wide = lax.optimization_barrier(
        (wide_table(ROT_BLOCK, ids), wide_table(HID_BLOCK, ids))
    )
    pair_rot = rotate_rows(
        jnp.concatenate([padded(gate_weight, 1), padded(up_weight, 1)], axis=1),
        ROT_BLOCK,
        rot_wide,
    )
    wide = pair_rot.shape[1] // 2
    down_rot = rotate_rows(padded(down_weight, 0), HID_BLOCK, hid_wide)
    token_rot = rotate_cols(tokens, ROT_BLOCK, rot_wide)
    tops = jnp.concatenate(
        [
            column_peaks(pair_rot[:, :wide]),
            column_peaks(pair_rot[:, wide:]),
            column_peaks(down_rot),
            column_peaks(token_rot),
        ],
        axis=0,
    )
    peaks = everyones(after(tops.max(axis=1), column))
    gate_peak, up_peak, down_peak, token_peak = peaks[0], peaks[1], peaks[2], peaks[3]
    pair_peak = jnp.where(jnp.arange(2 * wide) < wide, gate_peak, up_peak)[None, :]
    weight_pair = soft_cast(pair_rot, pair_peak)
    down_cast = soft_cast(down_rot, down_peak)

    mine_tokens, their_tokens = halves_along_x(blocks_along_x(token_column), first)
    mine_cot, their_cot = halves_along_x(blocks_along_x(cot_column), first)

    their_tok = soft_cast(rotate_cols(their_tokens, ROT_BLOCK, rot_wide), token_peak)
    mine_tok = soft_cast(rotate_cols(mine_tokens, ROT_BLOCK, rot_wide), token_peak)

    def part(tok, cot):
        return jnp.concatenate(
            [dot(tok, weight_pair, 1, 0) * 2.0**-12, dot(cot, down_cast, 1, 1) * 2.0**-6], axis=1
        )

    sums = scatter_width(part(mine_tok, mine_cot), part(their_tok, their_cot), f16)
    scales = jnp.stack(
        [
            token_peak * gate_peak / (fp_top * fp_top) * 2.0**12,
            token_peak * up_peak / (fp_top * fp_top) * 2.0**12,
            down_peak / fp_top * 2.0**6,
        ]
    )
    vmem = pl.BlockSpec(memory_space=pltpu.VMEM)
    acts, hidden_top = pl.pallas_call(
        middle_kernel,
        out_shape=(
            jax.ShapeDtypeStruct(sums.shape, bf16),
            jax.ShapeDtypeStruct((8, 128), f32),
        ),
        in_specs=[vmem] * 3,
        out_specs=(vmem, vmem),
        name="middle",
    )(sums, jnp.broadcast_to(scales[:, None], (3, wide)), hid_wide[:128, :128])
    mine_acts, their_acts = gather_half(acts)
    mine_act, their_act = mine_acts[:, : 2 * wide], their_acts[:, : 2 * wide]
    mine_hid, their_hid = mine_acts[:, 2 * wide :], their_acts[:, 2 * wide :]

    hidden_tops = copied(hidden_top.max(axis=0, keepdims=True), ALL, NY * NC * NZ * NX)

    def in_part(half):
        return dot(half[:, :wide], weight_pair[:, :wide], 1, 1) * (gate_peak / fp_top) + dot(
            half[:, wide:], weight_pair[:, wide:], 1, 1
        ) * (up_peak / fp_top)

    mine_in, their_in = in_part(mine_act), in_part(their_act)
    in_column, in_sends = sum_along_x(mine_in, their_in, first, bf16)

    hidden_peak = after(hidden_tops, in_sends).max()

    def out_part(half):
        cast = soft_cast(rotate_cols(half, HID_BLOCK, hid_wide), hidden_peak)
        return cast, dot(cast, down_cast, 1, 0) * 2.0**-13

    (mine_hid_cast, mine_out), (their_hid_cast, their_out) = (
        out_part(mine_hid),
        out_part(their_hid),
    )
    out_column, out_sends = sum_along_x(mine_out, their_out, first, f16)

    in_arrived = pieces_along_z(in_column)
    input_sum = in_arrived.astype(f32).sum(axis=0)
    input_grad = rotate_cols(input_sum, ROT_BLOCK).astype(bf16)
    out_arrived = pieces_along_z(after(out_column, in_arrived))
    out_sum = out_arrived.astype(f32).sum(axis=0)
    output = (out_sum * (hidden_peak * down_peak / (fp_top * fp_top) * 2.0**13)).astype(bf16)

    mine_hid_cast, their_hid_cast = after((mine_hid_cast, their_hid_cast), out_sends)
    down_dot = dot(mine_hid_cast, mine_cot, 0, 0) + dot(their_hid_cast, their_cot, 0, 0)
    down_grad = rotate_rows_split(down_dot * (hidden_peak / fp_top), HID_BLOCK, hid_wide)
    down_grad = down_grad[:hid].astype(bf16)
    mine_act, their_act = after((mine_act, their_act), in_column)
    pair_dot = dot(mine_tok, mine_act, 0, 0) + dot(their_tok, their_act, 0, 0)
    pair_grad = rotate_rows_split(pair_dot * (token_peak / fp_top), ROT_BLOCK, rot_wide)
    pair_grad = row_major(pair_grad.astype(bf16))
    return (
        output,
        input_grad,
        pair_grad[:, :hid],
        pair_grad[:, wide : wide + hid],
        down_grad,
    )


def solution(mesh):
    split = Mesh(mesh.devices.reshape(NY, NC, NZ, NX), ALL)
    placed = (P(GY, GX), P(GY, GX), P(GX, GY), P(GX, GY), P(GY, GX))
    return jax.shard_map(
        layer,
        mesh=split,
        in_specs=placed,
        out_specs=(P(GY, GX), P(GY, GX), P(GX, GY), P(GX, GY), P(GY, GX)),
        check_vma=False,
    )
```

```python
import jax
import jax.numpy as jnp
from jax import lax
from jax.experimental import pallas as pl
from jax.experimental.pallas import tpu as pltpu
from jax.sharding import Mesh
from jax.sharding import PartitionSpec as P


ROT_BLOCK = 128
HID_BLOCK = 64
NY, NC, NZ, NX = 4, 2, 8, 4
GX = ("y", "c")
GY = ("z", "x")
ALL = ("y", "c", "z", "x")


fp_top = 448.0
tiny = 1e-06
bf16 = jnp.bfloat16
f16 = jnp.float16
f32 = jnp.float32


def hadamard_table(block_size):
    row_ids = jnp.arange(block_size, dtype=jnp.int32)[:, None]
    col_ids = jnp.arange(block_size, dtype=jnp.int32)[None, :]
    shared = row_ids & col_ids
    parity = jnp.zeros((block_size, block_size), jnp.int32)
    for bit_pos in range(max(block_size.bit_length() - 1, 1)):
        parity = parity + (shared >> bit_pos & 1)
    return (1 - 2 * (parity % 2)).astype(f32)


def wide_table(block_size, i):
    parity = jnp.zeros((i.shape[0], i.shape[0]), jnp.int32)
    shared = i[:, None] & i[None, :]
    for bit_pos in range(block_size.bit_length() - 1):
        parity = parity + (shared >> bit_pos & 1)
    same = i[:, None] // block_size == i[None, :] // block_size
    return jnp.where(same, 1 - 2 * (parity % 2), 0).astype(bf16)


def rotate_cols(matrix, block_size, wide=None):
    row_total, col_total = matrix.shape
    table = hadamard_table(block_size)
    if wide is not None:
        turned = dot(matrix, wide, 1, 0)
    else:
        blocks = matrix.reshape(row_total, col_total // block_size, block_size)
        turned = jnp.einsum("rbk,kl->rbl", blocks, table, precision=lax.Precision.HIGHEST)
    return turned.reshape(row_total, col_total) * block_size ** (-0.5)


def rotate_rows(matrix, block_size, wide=None):
    row_total, col_total = matrix.shape
    table = hadamard_table(block_size)
    if wide is not None:
        turned = dot(wide, matrix, 1, 0)
    else:
        blocks = matrix.reshape(row_total // block_size, block_size, col_total)
        turned = jnp.einsum("kl,bkc->blc", table, blocks, precision=lax.Precision.HIGHEST)
    return turned.reshape(row_total, col_total) * block_size ** (-0.5)


def soft_cast(values, top):
    return (fp_top * jnp.tanh(values / (top + tiny))).astype(bf16)


def dot(left, right, left_dim, right_dim):
    return lax.dot_general(
        left, right, (((left_dim,), (right_dim,)), ((), ())), preferred_element_type=f32
    )


def after(values, *earlier):
    return lax.optimization_barrier((values, earlier))[0]


def swapped(value):
    return lax.ppermute(value, "c", [(0, 1), (1, 0)])


def shifted(value, axis, size, step):
    return lax.ppermute(value, axis, [(i, (i + step) % size) for i in range(size)])


def along_x(value, step, back=False):
    pairs = []
    for c in range(NC):
        for x in range(NX):
            to = c * NX + (x + (step if c == 0 else -step)) % NX
            pairs.append((to, c * NX + x) if back else (c * NX + x, to))
    return lax.ppermute(value, ("c", "x"), pairs)


def copied(value, axes, count):
    return lax.all_to_all(jnp.broadcast_to(value, (count, *value.shape)), axes, 0, 0, tiled=True)


def blocks_along_x(column):
    return column, shifted(column, "x", NX, 2), along_x(column, 1), along_x(column, 3)


def halves_along_x(blocks, first):
    column, far, near, last = blocks
    mine = jnp.concatenate([jnp.where(first, column, far), near], axis=0)
    other = jnp.concatenate([jnp.where(first, far, column), last], axis=0)
    return mine, other


def sum_along_x(keep, far, near, last):
    near = along_x(near, 1, back=True)
    last = along_x(last, 3, back=True)
    far = shifted(far, "x", NX, 2)
    total = keep + near.astype(f32) + last.astype(f32) + far.astype(f32)
    return total.astype(bf16)


def pieces_along_z(column):
    pieces = column.reshape(NZ, column.shape[0] // NZ, column.shape[1])
    return lax.all_to_all(pieces, "z", 0, 0, tiled=True)


def scatter_width(mine, theirs, kind):
    got = swapped(theirs.astype(kind))
    blocks = (mine + got.astype(f32)).reshape(NY, mine.shape[0] // NY, mine.shape[1])
    me = lax.axis_index("y")
    total = lax.dynamic_index_in_dim(blocks, me, 0, keepdims=False)
    sends = [
        lax.dynamic_index_in_dim(blocks, (me + step) % NY, 0, keepdims=False).astype(kind)
        for step in range(1, NY)
    ]
    for step in range(1, NY):
        total = total + shifted(sends[step - 1], "y", NY, step).astype(f32)
    return total


def join_kernel(me_ref, own_ref, got1_ref, got2_ref, got3_ref, out_ref):
    rows = own_ref.shape[0]
    for step, ref in enumerate((own_ref, got1_ref, got2_ref, got3_ref)):
        at = pl.multiple_of(((me_ref[0] + NY - step) & (NY - 1)) * rows, rows)
        out_ref[pl.ds(at, rows), :] = ref[...]


def gather_half(value):
    got = [shifted(value, "y", NY, step) for step in range(1, NY)]
    vmem = pl.BlockSpec(memory_space=pltpu.VMEM)
    mine = pl.pallas_call(
        join_kernel,
        out_shape=jax.ShapeDtypeStruct((NY * value.shape[0], value.shape[1]), value.dtype),
        in_specs=[pl.BlockSpec(memory_space=pltpu.SMEM)] + [vmem] * NY,
        out_specs=vmem,
        name="join",
    )(lax.axis_index("y")[None], value, *got)
    return mine, swapped(mine)


def middle_kernel(sums_ref, scales_ref, table_ref, out_ref, top_ref):
    wide = scales_ref.shape[1]
    table = table_ref[...]
    top = jnp.zeros((8, 128), f32)
    for at in range(0, wide, 128):
        gate = sums_ref[:, at : at + 128] * scales_ref[0:1, at : at + 128]
        up = sums_ref[:, wide + at : wide + at + 128] * scales_ref[1:2, at : at + 128]
        back = sums_ref[:, 2 * wide + at : 2 * wide + at + 128] * scales_ref[2:3, at : at + 128]
        sig = jax.nn.sigmoid(gate)
        hidden = (gate * sig * up).astype(bf16)
        turned = jnp.abs(jnp.dot(hidden, table, preferred_element_type=f32)) * HID_BLOCK**-0.5
        for row in range(0, turned.shape[0], 8):
            top = jnp.maximum(top, turned[row : row + 8])
        grad = jnp.zeros(back.shape, f32)
        for _ in range(3):
            term = back.astype(bf16)
            grad = grad + jnp.dot(term, table, preferred_element_type=f32)
            back = back - term.astype(f32)
        grad = grad * HID_BLOCK**-0.5
        gate_act = grad * up * sig * (1.0 + gate * (1.0 - sig))
        out_ref[:, at : at + 128] = gate_act.astype(bf16)
        out_ref[:, wide + at : wide + at + 128] = (grad * gate * sig).astype(bf16)
        out_ref[:, 2 * wide + at : 2 * wide + at + 128] = hidden
    top_ref[...] = top


def in_kernel(core_ref, scale_ref, mine_ref, their_ref, pair_ref, keep_ref, far_ref, near_ref, last_ref):
    rows, wide = keep_ref.shape[0], pair_ref.shape[0] // 2
    first = core_ref[0] == 0

    def product(acts):
        gate = dot(acts[:, :wide], pair_ref[:wide, :], 1, 0) * scale_ref[0]
        return gate + dot(acts[:, wide:], pair_ref[wide:, :], 1, 0) * scale_ref[1]

    near_ref[...] = product(mine_ref[rows:, : 2 * wide]).astype(bf16)
    last_ref[...] = product(their_ref[rows:, : 2 * wide]).astype(bf16)
    mine, their = mine_ref[:rows, : 2 * wide], their_ref[:rows, : 2 * wide]
    far_ref[...] = product(jnp.where(first, their, mine)).astype(bf16)
    keep_ref[...] = product(jnp.where(first, mine, their))


def out_kernel(
    core_ref, scale_ref, mine_ref, their_ref, table_ref, down_ref,
    keep_ref, far_ref, near_ref, last_ref, mine_cast_ref, their_cast_ref,
):
    rows, wide = keep_ref.shape[0], down_ref.shape[0]
    first = core_ref[0] == 0
    table = table_ref[...]
    for half_ref, cast_ref in ((mine_ref, mine_cast_ref), (their_ref, their_cast_ref)):
        for at in range(0, wide, 128):
            block = half_ref[:, 2 * wide + at : 2 * wide + at + 128]
            turned = jnp.dot(block, table, preferred_element_type=f32) * scale_ref[0]
            cast_ref[:, at : at + 128] = (fp_top * jnp.tanh(turned)).astype(bf16)
    down = down_ref[...]
    near_ref[...] = dot(mine_cast_ref[rows:, :], down, 1, 0).astype(bf16)
    last_ref[...] = dot(their_cast_ref[rows:, :], down, 1, 0).astype(bf16)
    mine, their = mine_cast_ref[:rows, :], their_cast_ref[:rows, :]
    far_ref[...] = dot(jnp.where(first, their, mine), down, 1, 0).astype(bf16)
    keep_ref[...] = dot(jnp.where(first, mine, their), down, 1, 0)


def four_parts(rows, width):
    return [jax.ShapeDtypeStruct((rows, width), f32)] + [
        jax.ShapeDtypeStruct((rows, width), bf16)
    ] * 3


def padded(array, dim):
    extra = -array.shape[dim] % 128
    widths = [(0, extra if d == dim else 0) for d in range(array.ndim)]
    return jnp.pad(array, widths)


def column_peaks(values):
    return jnp.max(jnp.abs(values), axis=0, keepdims=True)


def everyones(values):
    copies = jnp.broadcast_to(values, (NY * NC * NZ * NX, 1, values.shape[0]))
    return lax.all_to_all(copies, ALL, 0, 0, tiled=True).max(axis=(0, 1))


def rotate_split(matrix, block_size, wide, rows):
    total = 0.0
    for _ in range(3):
        term = lax.reduce_precision(matrix, 8, 7)
        part = term.astype(bf16)
        total = total + (dot(wide, part, 1, 0) if rows else dot(part, wide, 1, 0))
        matrix = matrix - term
    return total * block_size ** (-0.5)


def layer(tokens, cotangent, gate_weight, up_weight, down_weight):
    hid = gate_weight.shape[1]
    rows, features = tokens.shape
    core = lax.axis_index("c")
    first = core == 0

    column = copied(jnp.concatenate([tokens, cotangent], axis=0), "z", NZ)
    token_column = column[:, :rows].reshape(NZ * rows, features)
    cot_column = column[:, rows:].reshape(NZ * rows, features)

    ids = lax.optimization_barrier(jnp.arange(features, dtype=jnp.int32))
    rot_wide, hid_wide = lax.optimization_barrier(
        (wide_table(ROT_BLOCK, ids), wide_table(HID_BLOCK, ids))
    )
    pair_rot = rotate_cols(
        jnp.concatenate([padded(gate_weight.T, 0), padded(up_weight.T, 0)], axis=0),
        ROT_BLOCK,
        rot_wide,
    )
    wide = pair_rot.shape[0] // 2
    down_rot = rotate_rows(padded(down_weight, 0), HID_BLOCK, hid_wide)
    token_rot = rotate_cols(tokens, ROT_BLOCK, rot_wide)
    tops = jnp.concatenate(
        [
            column_peaks(pair_rot[:wide]),
            column_peaks(pair_rot[wide:]),
            column_peaks(down_rot),
            column_peaks(token_rot),
        ],
        axis=0,
    )
    peaks = everyones(after(tops.max(axis=1), column))
    gate_peak, up_peak, down_peak, token_peak = peaks[0], peaks[1], peaks[2], peaks[3]
    pair_peak = jnp.where(jnp.arange(2 * wide) < wide, gate_peak, up_peak)[:, None]
    weight_pair = soft_cast(pair_rot, pair_peak)
    down_cast = soft_cast(down_rot, down_peak)

    mine_tokens, their_tokens = halves_along_x(blocks_along_x(token_column), first)
    cot_blocks = blocks_along_x(cot_column)

    their_tok = soft_cast(rotate_cols(their_tokens, ROT_BLOCK, rot_wide), token_peak)
    mine_tok = soft_cast(rotate_cols(mine_tokens, ROT_BLOCK, rot_wide), token_peak)

    mine_pair = dot(mine_tok, weight_pair, 1, 1) * 2.0**-12
    their_pair = (dot(their_tok, weight_pair, 1, 1) * 2.0**-12).astype(f16)
    mine_cot, their_cot = halves_along_x(after(cot_blocks, mine_pair, their_pair), first)
    their_back = (dot(their_cot, down_cast, 1, 1) * 2.0**-6).astype(f16)
    mine_back = dot(mine_cot, down_cast, 1, 1) * 2.0**-6
    sums = scatter_width(
        jnp.concatenate([mine_pair, mine_back], axis=1),
        jnp.concatenate([their_pair, their_back], axis=1),
        f16,
    )
    scales = jnp.stack(
        [
            token_peak * gate_peak / (fp_top * fp_top) * 2.0**12,
            token_peak * up_peak / (fp_top * fp_top) * 2.0**12,
            down_peak / fp_top * 2.0**6,
        ]
    )
    vmem = pl.BlockSpec(memory_space=pltpu.VMEM)
    acts, hidden_top = pl.pallas_call(
        middle_kernel,
        out_shape=(
            jax.ShapeDtypeStruct(sums.shape, bf16),
            jax.ShapeDtypeStruct((8, 128), f32),
        ),
        in_specs=[vmem] * 3,
        out_specs=(vmem, vmem),
        name="middle",
    )(sums, jnp.broadcast_to(scales[:, None], (3, wide)), hid_wide[:128, :128])
    mine_acts, their_acts = gather_half(acts)

    hidden_tops = copied(hidden_top.max(axis=0, keepdims=True), ALL, NY * NC * NZ * NX)

    smem = pl.BlockSpec(memory_space=pltpu.SMEM)
    quarter = mine_acts.shape[0] // 2
    in_parts = pl.pallas_call(
        in_kernel,
        out_shape=four_parts(quarter, features),
        in_specs=[smem] * 2 + [vmem] * 3,
        out_specs=[vmem] * 4,
        name="in_part",
    )(core[None], peaks[:2] / fp_top, mine_acts, their_acts, weight_pair)
    in_column = sum_along_x(*in_parts)

    hidden_peak = after(hidden_tops, *in_parts).max()
    *out_parts, mine_hid_cast, their_hid_cast = pl.pallas_call(
        out_kernel,
        out_shape=four_parts(quarter, features)
        + [jax.ShapeDtypeStruct((2 * quarter, wide), bf16)] * 2,
        in_specs=[smem] * 2 + [vmem] * 4,
        out_specs=[vmem] * 6,
        name="out_part",
    )(
        core[None],
        (HID_BLOCK**-0.5 / (hidden_peak + tiny))[None],
        mine_acts,
        their_acts,
        hid_wide[:128, :128],
        down_cast,
    )
    out_column = sum_along_x(*out_parts)

    in_arrived = pieces_along_z(in_column)
    input_sum = in_arrived.astype(f32).sum(axis=0)
    input_grad = rotate_cols(input_sum, ROT_BLOCK).astype(bf16)
    out_arrived = pieces_along_z(after(out_column, in_arrived))
    out_sum = out_arrived.astype(f32).sum(axis=0)
    output = (out_sum * (hidden_peak * down_peak / (fp_top * fp_top))).astype(bf16)

    mine_hid_cast, their_hid_cast = after((mine_hid_cast, their_hid_cast), out_parts, in_column)
    down_dot = dot(mine_hid_cast, mine_cot, 0, 0) + dot(their_hid_cast, their_cot, 0, 0)
    down_grad = rotate_split(down_dot * (hidden_peak / fp_top), HID_BLOCK, hid_wide, True)
    down_grad = down_grad[:hid].astype(bf16)
    mine_tok, their_tok = after((mine_tok, their_tok), out_parts, in_column)
    pair_dot = dot(mine_acts[:, : 2 * wide], mine_tok, 0, 0) + dot(
        their_acts[:, : 2 * wide], their_tok, 0, 0
    )
    pair_grad = rotate_split(pair_dot * (token_peak / fp_top), ROT_BLOCK, rot_wide, False)
    pair_grad = pair_grad.astype(bf16)
    return (
        output,
        input_grad,
        pair_grad[:hid].T,
        pair_grad[wide : wide + hid].T,
        down_grad,
    )


def solution(mesh):
    split = Mesh(mesh.devices.reshape(NY, NC, NZ, NX), ALL)
    placed = (P(GY, GX), P(GY, GX), P(GX, GY), P(GX, GY), P(GY, GX))
    return jax.shard_map(
        layer,
        mesh=split,
        in_specs=placed,
        out_specs=(P(GY, GX), P(GY, GX), P(GX, GY), P(GX, GY), P(GY, GX)),
        check_vma=False,
    )
```

```python
import jax
import jax.numpy as jnp
from jax import lax
from jax.experimental import pallas as pl
from jax.experimental.pallas import tpu as pltpu
from jax.sharding import Mesh
from jax.sharding import PartitionSpec as P


ROT_BLOCK = 128
HID_BLOCK = 64
NY, NC, NZ, NX = 4, 2, 8, 4
GX = ("y", "c")
GY = ("z", "x")
ALL = ("y", "c", "z", "x")


fp_top = 448.0
tiny = 1e-06
bf16 = jnp.bfloat16
f16 = jnp.float16
f32 = jnp.float32


def hadamard_table(block_size):
    row_ids = jnp.arange(block_size, dtype=jnp.int32)[:, None]
    col_ids = jnp.arange(block_size, dtype=jnp.int32)[None, :]
    shared = row_ids & col_ids
    parity = jnp.zeros((block_size, block_size), jnp.int32)
    for bit_pos in range(max(block_size.bit_length() - 1, 1)):
        parity = parity + (shared >> bit_pos & 1)
    return (1 - 2 * (parity % 2)).astype(f32)


def wide_table(block_size, i):
    parity = jnp.zeros((i.shape[0], i.shape[0]), jnp.int32)
    shared = i[:, None] & i[None, :]
    for bit_pos in range(block_size.bit_length() - 1):
        parity = parity + (shared >> bit_pos & 1)
    same = i[:, None] // block_size == i[None, :] // block_size
    return jnp.where(same, 1 - 2 * (parity % 2), 0).astype(bf16)


def rotate_cols(matrix, block_size, wide=None):
    row_total, col_total = matrix.shape
    table = hadamard_table(block_size)
    if wide is not None:
        turned = dot(matrix, wide, 1, 0)
    else:
        blocks = matrix.reshape(row_total, col_total // block_size, block_size)
        turned = jnp.einsum("rbk,kl->rbl", blocks, table, precision=lax.Precision.HIGHEST)
    return turned.reshape(row_total, col_total) * block_size ** (-0.5)


def rotate_rows(matrix, block_size, wide=None):
    row_total, col_total = matrix.shape
    table = hadamard_table(block_size)
    if wide is not None:
        turned = dot(wide, matrix, 1, 0)
    else:
        blocks = matrix.reshape(row_total // block_size, block_size, col_total)
        turned = jnp.einsum("kl,bkc->blc", table, blocks, precision=lax.Precision.HIGHEST)
    return turned.reshape(row_total, col_total) * block_size ** (-0.5)


def soft_cast(values, top):
    return (fp_top * jnp.tanh(values / (top + tiny))).astype(bf16)


def dot(left, right, left_dim, right_dim):
    return lax.dot_general(
        left, right, (((left_dim,), (right_dim,)), ((), ())), preferred_element_type=f32
    )


def after(values, *earlier):
    return lax.optimization_barrier((values, earlier))[0]


def swapped(value):
    return lax.ppermute(value, "c", [(0, 1), (1, 0)])


def shifted(value, axis, size, step):
    return lax.ppermute(value, axis, [(i, (i + step) % size) for i in range(size)])


def along_x(value, step, back=False):
    pairs = []
    for c in range(NC):
        for x in range(NX):
            to = c * NX + (x + (step if c == 0 else -step)) % NX
            pairs.append((to, c * NX + x) if back else (c * NX + x, to))
    return lax.ppermute(value, ("c", "x"), pairs)


def copied(value, axes, count):
    return lax.all_to_all(jnp.broadcast_to(value, (count, *value.shape)), axes, 0, 0, tiled=True)


def blocks_along_x(column):
    return column, shifted(column, "x", NX, 2), along_x(column, 1), along_x(column, 3)


def halves_along_x(blocks, first):
    column, far, near, last = blocks
    mine = jnp.concatenate([jnp.where(first, column, far), near], axis=0)
    other = jnp.concatenate([jnp.where(first, far, column), last], axis=0)
    return mine, other


def sum_along_x(keep, far, near, last):
    near = along_x(near, 1, back=True)
    last = along_x(last, 3, back=True)
    far = shifted(far, "x", NX, 2)
    total = keep + near.astype(f32) + last.astype(f32) + far.astype(f32)
    return total.astype(bf16)


def pieces_along_z(column):
    pieces = column.reshape(NZ, column.shape[0] // NZ, column.shape[1])
    return lax.all_to_all(pieces, "z", 0, 0, tiled=True)


def sum_with_other_core(mine, theirs):
    total = mine + swapped(theirs).astype(f32)
    return total.reshape(NY, mine.shape[0] // NY, mine.shape[1])


def scatter_width(blocks, kind):
    me = lax.axis_index("y")

    def block(step):
        picked = [
            lax.dynamic_index_in_dim(b, (me + step) % NY, 0, keepdims=False) for b in blocks
        ]
        return jnp.concatenate(picked, axis=1)

    sends = [block(step).astype(kind) for step in range(1, NY)]
    total = block(0)
    for step in range(1, NY):
        total = total + shifted(sends[step - 1], "y", NY, step).astype(f32)
    return total


def join_kernel(me_ref, own_ref, got1_ref, got2_ref, got3_ref, out_ref):
    rows = own_ref.shape[0]
    for step, ref in enumerate((own_ref, got1_ref, got2_ref, got3_ref)):
        at = pl.multiple_of(((me_ref[0] + NY - step) & (NY - 1)) * rows, rows)
        out_ref[pl.ds(at, rows), :] = ref[...]


def gather_half(value):
    got = [shifted(value, "y", NY, step) for step in range(1, NY)]
    shape = (NY * value.shape[0], value.shape[1])
    (mine,) = call(
        join_kernel, [(shape, value.dtype)], [lax.axis_index("y")[None]], [value, *got], None
    )
    return mine, swapped(mine)


def middle_kernel(sums_ref, scales_ref, table_ref, out_ref, top_ref):
    wide = scales_ref.shape[1]
    table = table_ref[...]
    top = jnp.zeros((8, 128), f32)
    for at in range(0, wide, 128):
        gate = sums_ref[:, at : at + 128] * scales_ref[0:1, at : at + 128]
        up = sums_ref[:, wide + at : wide + at + 128] * scales_ref[1:2, at : at + 128]
        back = sums_ref[:, 2 * wide + at : 2 * wide + at + 128] * scales_ref[2:3, at : at + 128]
        sig = jax.nn.sigmoid(gate)
        hidden = (gate * sig * up).astype(bf16)
        turned = jnp.abs(jnp.dot(hidden, table, preferred_element_type=f32)) * HID_BLOCK**-0.5
        for row in range(0, turned.shape[0], 8):
            top = jnp.maximum(top, turned[row : row + 8])
        grad = jnp.zeros(back.shape, f32)
        for _ in range(3):
            term = back.astype(bf16)
            grad = grad + jnp.dot(term, table, preferred_element_type=f32)
            back = back - term.astype(f32)
        grad = grad * HID_BLOCK**-0.5
        gate_act = grad * up * sig * (1.0 + gate * (1.0 - sig))
        out_ref[:, at : at + 128] = gate_act.astype(bf16)
        out_ref[:, wide + at : wide + at + 128] = (grad * gate * sig).astype(bf16)
        out_ref[:, 2 * wide + at : 2 * wide + at + 128] = hidden
    top_ref[...] = top


def in_product(acts, pair_ref, scale_ref):
    wide = pair_ref.shape[0] // 2
    gate = dot(acts[:, :wide], pair_ref[:wide, :], 1, 0) * scale_ref[0]
    return gate + dot(acts[:, wide:], pair_ref[wide:, :], 1, 0) * scale_ref[1]


def place_parts(first, mine, their, keep_ref, far_ref):
    far_ref[...] = jnp.where(first, their, mine).astype(bf16)
    keep_ref[...] = jnp.where(first, mine, their)


def in_mine_kernel(scale_ref, acts_ref, pair_ref, part_ref, near_ref):
    rows, both = part_ref.shape[0], pair_ref.shape[0]
    near_ref[...] = in_product(acts_ref[rows:, :both], pair_ref, scale_ref).astype(bf16)
    part_ref[...] = in_product(acts_ref[:rows, :both], pair_ref, scale_ref)


def in_their_kernel(
    core_ref, scale_ref, acts_ref, pair_ref, part_ref, keep_ref, far_ref, last_ref
):
    rows, both = part_ref.shape[0], pair_ref.shape[0]
    last_ref[...] = in_product(acts_ref[rows:, :both], pair_ref, scale_ref).astype(bf16)
    their = in_product(acts_ref[:rows, :both], pair_ref, scale_ref)
    place_parts(core_ref[0] == 0, part_ref[...], their, keep_ref, far_ref)


def cast_hidden(tops_ref, acts_ref, table_ref, cast_ref):
    table, wide = table_ref[...], cast_ref.shape[1]
    top = jnp.max(jnp.max(tops_ref[...], axis=0, keepdims=True))
    scale = HID_BLOCK**-0.5 / jnp.full((1, 128), top + tiny, f32)
    for at in range(0, wide, 128):
        block = acts_ref[:, 2 * wide + at : 2 * wide + at + 128]
        turned = jnp.dot(block, table, preferred_element_type=f32) * scale
        cast_ref[:, at : at + 128] = (fp_top * jnp.tanh(turned)).astype(bf16)
    return top


def out_mine_kernel(
    tops_ref, acts_ref, table_ref, down_ref, part_ref, near_ref, cast_ref, top_ref
):
    rows = part_ref.shape[0]
    top_ref[...] = jnp.full(top_ref.shape, cast_hidden(tops_ref, acts_ref, table_ref, cast_ref))
    near_ref[...] = dot(cast_ref[rows:, :], down_ref[...], 1, 0).astype(bf16)
    part_ref[...] = dot(cast_ref[:rows, :], down_ref[...], 1, 0)


def out_their_kernel(
    core_ref, tops_ref, acts_ref, table_ref, down_ref, part_ref,
    keep_ref, far_ref, last_ref, cast_ref,
):
    rows = part_ref.shape[0]
    cast_hidden(tops_ref, acts_ref, table_ref, cast_ref)
    last_ref[...] = dot(cast_ref[rows:, :], down_ref[...], 1, 0).astype(bf16)
    their = dot(cast_ref[:rows, :], down_ref[...], 1, 0)
    place_parts(core_ref[0] == 0, part_ref[...], their, keep_ref, far_ref)


def call(kernel, outs, scalars, arrays, limit=4 * 2**20):
    smem, vmem = pl.BlockSpec(memory_space=pltpu.SMEM), pl.BlockSpec(memory_space=pltpu.VMEM)
    return pl.pallas_call(
        kernel,
        out_shape=[jax.ShapeDtypeStruct(shape, kind) for shape, kind in outs],
        in_specs=[smem] * len(scalars) + [vmem] * len(arrays),
        out_specs=[vmem] * len(outs),
        compiler_params=pltpu.CompilerParams(vmem_limit_bytes=limit),
    )(*scalars, *arrays)


def padded(array, dim):
    extra = -array.shape[dim] % 128
    widths = [(0, extra if d == dim else 0) for d in range(array.ndim)]
    return jnp.pad(array, widths)


def column_peaks(values):
    return jnp.max(jnp.abs(values), axis=0, keepdims=True)


def everyones(values):
    copies = jnp.broadcast_to(values, (NY * NC * NZ * NX, 1, values.shape[0]))
    return lax.all_to_all(copies, ALL, 0, 0, tiled=True).max(axis=(0, 1))


def rotate_split(matrix, block_size, wide, rows):
    total = 0.0
    for _ in range(3):
        term = lax.reduce_precision(matrix, 8, 7)
        part = term.astype(bf16)
        total = total + (dot(wide, part, 1, 0) if rows else dot(part, wide, 1, 0))
        matrix = matrix - term
    return total * block_size ** (-0.5)


def layer(tokens, cotangent, gate_weight, up_weight, down_weight):
    hid = gate_weight.shape[1]
    rows, features = tokens.shape
    core = lax.axis_index("c")
    first = core == 0

    column = copied(jnp.concatenate([tokens, cotangent], axis=0), "z", NZ)
    token_column = column[:, :rows].reshape(NZ * rows, features)
    cot_column = column[:, rows:].reshape(NZ * rows, features)

    ids = lax.optimization_barrier(jnp.arange(features, dtype=jnp.int32))
    rot_wide, hid_wide = lax.optimization_barrier(
        (wide_table(ROT_BLOCK, ids), wide_table(HID_BLOCK, ids))
    )
    pair_rot = rotate_cols(
        jnp.concatenate([padded(gate_weight.T, 0), padded(up_weight.T, 0)], axis=0),
        ROT_BLOCK,
        rot_wide,
    )
    wide = pair_rot.shape[0] // 2
    down_rot = rotate_rows(padded(down_weight, 0), HID_BLOCK, hid_wide)
    token_rot = rotate_cols(tokens, ROT_BLOCK, rot_wide)
    tops = jnp.concatenate(
        [
            column_peaks(pair_rot[:wide]),
            column_peaks(pair_rot[wide:]),
            column_peaks(down_rot),
            column_peaks(token_rot),
        ],
        axis=0,
    )
    peaks = everyones(after(tops.max(axis=1), column))
    in_scales = peaks[:2] / fp_top
    small_table = after(hid_wide[:128, :128], column)
    gate_peak, up_peak, down_peak, token_peak = (peaks[k : k + 1, None] for k in range(4))
    pair_peak = jnp.where(jnp.arange(2 * wide)[:, None] < wide, gate_peak, up_peak)
    weight_pair = soft_cast(pair_rot, pair_peak)
    down_cast = soft_cast(down_rot, down_peak)

    mine_tokens, their_tokens = halves_along_x(blocks_along_x(token_column), first)
    cot_blocks = blocks_along_x(cot_column)

    their_tok = soft_cast(rotate_cols(their_tokens, ROT_BLOCK, rot_wide), token_peak)
    mine_tok = soft_cast(rotate_cols(mine_tokens, ROT_BLOCK, rot_wide), token_peak)

    their_pair = (dot(their_tok, weight_pair, 1, 1) * 2.0**-12).astype(f16)
    mine_pair = dot(mine_tok, weight_pair, 1, 1) * 2.0**-12
    pair_blocks = sum_with_other_core(mine_pair, their_pair)
    mine_cot, their_cot = halves_along_x(after(cot_blocks, pair_blocks, their_pair), first)
    their_back = (dot(their_cot, down_cast, 1, 1) * 2.0**-6).astype(f16)
    mine_back = dot(mine_cot, down_cast, 1, 1) * 2.0**-6
    back_blocks = sum_with_other_core(mine_back, their_back)
    sums = scatter_width([pair_blocks, back_blocks], f16)
    scales = jnp.concatenate(
        [
            token_peak * gate_peak / (fp_top * fp_top) * 2.0**12,
            token_peak * up_peak / (fp_top * fp_top) * 2.0**12,
            down_peak / fp_top * 2.0**6,
        ],
        axis=0,
    )
    acts, hidden_top = call(
        middle_kernel,
        [(sums.shape, bf16), ((8, 128), f32)],
        [],
        [sums, jnp.broadcast_to(scales, (3, wide)), small_table],
    )
    mine_acts, their_acts = gather_half(acts)

    hidden_tops = copied(hidden_top.max(axis=0, keepdims=True), ALL, NY * NC * NZ * NX)

    quarter = mine_acts.shape[0] // 2
    part, piece = ((quarter, features), f32), ((quarter, features), bf16)
    in_mine, near = call(in_mine_kernel, [part, piece], [in_scales], [mine_acts, weight_pair])
    keep, far, last = call(
        in_their_kernel,
        [part, piece, piece],
        [core[None], in_scales],
        [their_acts, weight_pair, in_mine],
    )
    in_column = sum_along_x(keep, far, near, last)

    hidden_tops = after(hidden_tops, keep, far, last).reshape(-1, 128)
    cast = ((2 * quarter, wide), bf16)
    out_mine, near, mine_hid_cast, hidden_peak = call(
        out_mine_kernel,
        [part, piece, cast, ((8, features), f32)],
        [],
        [hidden_tops, mine_acts, small_table, down_cast],
    )
    keep, far, last, their_hid_cast = call(
        out_their_kernel,
        [part, piece, piece, cast],
        [core[None]],
        [hidden_tops, their_acts, small_table, down_cast, out_mine],
    )
    out_column = sum_along_x(keep, far, near, last)
    hidden_peak = hidden_peak[:1]

    in_arrived = pieces_along_z(in_column)
    input_sum = in_arrived.astype(f32).sum(axis=0)
    input_grad = rotate_cols(input_sum, ROT_BLOCK).astype(bf16)
    out_arrived = pieces_along_z(after(out_column, in_arrived))
    out_sum = out_arrived.astype(f32).sum(axis=0)
    output = (out_sum * (hidden_peak * down_peak / (fp_top * fp_top))).astype(bf16)

    mine_hid_cast, their_hid_cast = after((mine_hid_cast, their_hid_cast), keep)
    down_dot = dot(mine_hid_cast, mine_cot, 0, 0) + dot(their_hid_cast, their_cot, 0, 0)
    down_grad = rotate_split(down_dot, HID_BLOCK, hid_wide, True) * (hidden_peak / fp_top)
    down_grad = down_grad[:hid].astype(bf16)
    mine_tok, their_tok = after((mine_tok, their_tok), keep, in_column)
    pair_dot = dot(mine_acts[:, : 2 * wide], mine_tok, 0, 0) + dot(
        their_acts[:, : 2 * wide], their_tok, 0, 0
    )
    pair_grad = rotate_split(pair_dot * (token_peak / fp_top), ROT_BLOCK, rot_wide, False)
    pair_grad = pair_grad.astype(bf16)
    return (
        output,
        input_grad,
        pair_grad[:hid].T,
        pair_grad[wide : wide + hid].T,
        down_grad,
    )


def solution(mesh):
    split = Mesh(mesh.devices.reshape(NY, NC, NZ, NX), ALL)
    placed = (P(GY, GX), P(GY, GX), P(GX, GY), P(GX, GY), P(GY, GX))
    return jax.shard_map(
        layer,
        mesh=split,
        in_specs=placed,
        out_specs=(P(GY, GX), P(GY, GX), P(GX, GY), P(GX, GY), P(GY, GX)),
        check_vma=False,
    )
```

```python
import jax
import jax.numpy as jnp
from jax import lax
from jax.experimental import pallas as pl
from jax.experimental.pallas import tpu as pltpu
from jax.sharding import Mesh
from jax.sharding import PartitionSpec as P


ROT_BLOCK = 128
HID_BLOCK = 64
NY, NC, NZ, NX = 4, 2, 8, 4
GX = ("y", "c")
GY = ("z", "x")
ALL = ("y", "c", "z", "x")


fp_top = 448.0
tiny = 1e-06
bf16 = jnp.bfloat16
f16 = jnp.float16
f32 = jnp.float32


def hadamard_table(block_size):
    row_ids = jnp.arange(block_size, dtype=jnp.int32)[:, None]
    col_ids = jnp.arange(block_size, dtype=jnp.int32)[None, :]
    shared = row_ids & col_ids
    parity = jnp.zeros((block_size, block_size), jnp.int32)
    for bit_pos in range(max(block_size.bit_length() - 1, 1)):
        parity = parity + (shared >> bit_pos & 1)
    return (1 - 2 * (parity % 2)).astype(f32)


def wide_table(block_size, i):
    parity = jnp.zeros((i.shape[0], i.shape[0]), jnp.int32)
    shared = i[:, None] & i[None, :]
    for bit_pos in range(block_size.bit_length() - 1):
        parity = parity + (shared >> bit_pos & 1)
    same = i[:, None] // block_size == i[None, :] // block_size
    return jnp.where(same, 1 - 2 * (parity % 2), 0).astype(bf16)


def rotate_cols(matrix, block_size, wide=None):
    row_total, col_total = matrix.shape
    table = hadamard_table(block_size)
    if wide is not None:
        turned = dot(matrix, wide, 1, 0)
    else:
        blocks = matrix.reshape(row_total, col_total // block_size, block_size)
        turned = jnp.einsum("rbk,kl->rbl", blocks, table, precision=lax.Precision.HIGHEST)
    return turned.reshape(row_total, col_total) * block_size ** (-0.5)


def rotate_rows(matrix, block_size, wide=None):
    row_total, col_total = matrix.shape
    table = hadamard_table(block_size)
    if wide is not None:
        turned = dot(wide, matrix, 1, 0)
    else:
        blocks = matrix.reshape(row_total // block_size, block_size, col_total)
        turned = jnp.einsum("kl,bkc->blc", table, blocks, precision=lax.Precision.HIGHEST)
    return turned.reshape(row_total, col_total) * block_size ** (-0.5)


def soft_cast(values, top):
    return (fp_top * jnp.tanh(values / (top + tiny))).astype(bf16)


def dot(left, right, left_dim, right_dim):
    return lax.dot_general(
        left, right, (((left_dim,), (right_dim,)), ((), ())), preferred_element_type=f32
    )


def after(values, *earlier):
    return lax.optimization_barrier((values, earlier))[0]


def swapped(value):
    return lax.ppermute(value, "c", [(0, 1), (1, 0)])


def shifted(value, axis, size, step):
    return lax.ppermute(value, axis, [(i, (i + step) % size) for i in range(size)])


def along_x(value, step, back=False):
    pairs = []
    for c in range(NC):
        for x in range(NX):
            to = c * NX + (x + (step if c == 0 else -step)) % NX
            pairs.append((to, c * NX + x) if back else (c * NX + x, to))
    return lax.ppermute(value, ("c", "x"), pairs)


def copied(value, axes, count):
    return lax.all_to_all(jnp.broadcast_to(value, (count, *value.shape)), axes, 0, 0, tiled=True)


def blocks_along_x(column):
    return column, shifted(column, "x", NX, 2), along_x(column, 1), along_x(column, 3)


def halves_along_x(blocks, first):
    column, far, near, last = blocks
    mine = jnp.concatenate([jnp.where(first, column, far), near], axis=0)
    other = jnp.concatenate([jnp.where(first, far, column), last], axis=0)
    return mine, other


def sum_along_x(keep, far, near, last):
    near = along_x(near, 1, back=True)
    last = along_x(last, 3, back=True)
    far = shifted(far, "x", NX, 2)
    total = keep + near.astype(f32) + last.astype(f32) + far.astype(f32)
    return total.astype(bf16)


def pieces_along_z(column):
    pieces = column.reshape(NZ, column.shape[0] // NZ, column.shape[1])
    return lax.all_to_all(pieces, "z", 0, 0, tiled=True)


def sum_with_other_core(mine, theirs):
    total = mine + swapped(theirs).astype(f32)
    return total.reshape(NY, mine.shape[0] // NY, mine.shape[1])


def scatter_width(blocks, kind):
    me = lax.axis_index("y")

    def block(step):
        return lax.dynamic_index_in_dim(blocks, (me + step) % NY, 0, keepdims=False)

    sends = [block(step).astype(kind) for step in range(1, NY)]
    total = block(0)
    for step in range(1, NY):
        total = total + shifted(sends[step - 1], "y", NY, step).astype(f32)
    return total, sends


def join_kernel(me_ref, own_ref, got1_ref, got2_ref, got3_ref, out_ref):
    rows = own_ref.shape[0]
    for step, ref in enumerate((own_ref, got1_ref, got2_ref, got3_ref)):
        at = pl.multiple_of(((me_ref[0] + NY - step) & (NY - 1)) * rows, rows)
        out_ref[pl.ds(at, rows), :] = ref[...]


def gather_half(value):
    got = [shifted(value, "y", NY, step) for step in range(1, NY)]
    shape = (NY * value.shape[0], value.shape[1])
    (mine,) = call(
        join_kernel, [(shape, value.dtype)], [lax.axis_index("y")[None]], [value, *got], None
    )
    return mine, swapped(mine)


def middle_kernel(pair_ref, back_ref, scales_ref, table_ref, out_ref, top_ref):
    wide = scales_ref.shape[1]
    table = table_ref[...]
    top = jnp.zeros((8, 128), f32)
    for at in range(0, wide, 128):
        gate = pair_ref[:, at : at + 128] * scales_ref[0:1, at : at + 128]
        up = pair_ref[:, wide + at : wide + at + 128] * scales_ref[1:2, at : at + 128]
        back = back_ref[:, at : at + 128] * scales_ref[2:3, at : at + 128]
        sig = jax.nn.sigmoid(gate)
        hidden = (gate * sig * up).astype(bf16)
        turned = jnp.abs(jnp.dot(hidden, table, preferred_element_type=f32)) * HID_BLOCK**-0.5
        for row in range(0, turned.shape[0], 8):
            top = jnp.maximum(top, turned[row : row + 8])
        grad = jnp.zeros(back.shape, f32)
        for _ in range(3):
            term = back.astype(bf16)
            grad = grad + jnp.dot(term, table, preferred_element_type=f32)
            back = back - term.astype(f32)
        grad = grad * HID_BLOCK**-0.5
        gate_act = grad * up * sig * (1.0 + gate * (1.0 - sig))
        out_ref[:, at : at + 128] = gate_act.astype(bf16)
        out_ref[:, wide + at : wide + at + 128] = (grad * gate * sig).astype(bf16)
        out_ref[:, 2 * wide + at : 2 * wide + at + 128] = hidden
    top_ref[...] = top


def in_product(acts, pair_ref, scale_ref):
    wide = pair_ref.shape[0] // 2
    gate = dot(acts[:, :wide], pair_ref[:wide, :], 1, 0) * scale_ref[0]
    return gate + dot(acts[:, wide:], pair_ref[wide:, :], 1, 0) * scale_ref[1]


def place_parts(first, mine, their, keep_ref, far_ref):
    far_ref[...] = jnp.where(first, their, mine).astype(bf16)
    keep_ref[...] = jnp.where(first, mine, their)


def in_mine_kernel(scale_ref, acts_ref, pair_ref, part_ref, near_ref):
    rows, both = part_ref.shape[0], pair_ref.shape[0]
    near_ref[...] = in_product(acts_ref[rows:, :both], pair_ref, scale_ref).astype(bf16)
    part_ref[...] = in_product(acts_ref[:rows, :both], pair_ref, scale_ref)


def in_their_kernel(
    core_ref, scale_ref, acts_ref, pair_ref, part_ref, keep_ref, far_ref, last_ref
):
    rows, both = part_ref.shape[0], pair_ref.shape[0]
    last_ref[...] = in_product(acts_ref[rows:, :both], pair_ref, scale_ref).astype(bf16)
    their = in_product(acts_ref[:rows, :both], pair_ref, scale_ref)
    place_parts(core_ref[0] == 0, part_ref[...], their, keep_ref, far_ref)


def cast_hidden(tops_ref, acts_ref, table_ref, cast_ref):
    table, wide = table_ref[...], cast_ref.shape[1]
    top = jnp.max(jnp.max(tops_ref[...], axis=0, keepdims=True))
    scale = HID_BLOCK**-0.5 / jnp.full((1, 128), top + tiny, f32)
    for at in range(0, wide, 128):
        block = acts_ref[:, 2 * wide + at : 2 * wide + at + 128]
        turned = jnp.dot(block, table, preferred_element_type=f32) * scale
        cast_ref[:, at : at + 128] = (fp_top * jnp.tanh(turned)).astype(bf16)
    return top


def out_mine_kernel(
    tops_ref, acts_ref, table_ref, down_ref, part_ref, near_ref, cast_ref, top_ref
):
    rows = part_ref.shape[0]
    top_ref[...] = jnp.full(top_ref.shape, cast_hidden(tops_ref, acts_ref, table_ref, cast_ref))
    near_ref[...] = dot(cast_ref[rows:, :], down_ref[...], 1, 0).astype(bf16)
    part_ref[...] = dot(cast_ref[:rows, :], down_ref[...], 1, 0)


def out_their_kernel(
    core_ref, tops_ref, acts_ref, table_ref, down_ref, part_ref,
    keep_ref, far_ref, last_ref, cast_ref,
):
    rows = part_ref.shape[0]
    cast_hidden(tops_ref, acts_ref, table_ref, cast_ref)
    last_ref[...] = dot(cast_ref[rows:, :], down_ref[...], 1, 0).astype(bf16)
    their = dot(cast_ref[:rows, :], down_ref[...], 1, 0)
    place_parts(core_ref[0] == 0, part_ref[...], their, keep_ref, far_ref)


def call(kernel, outs, scalars, arrays, limit=4 * 2**20):
    smem, vmem = pl.BlockSpec(memory_space=pltpu.SMEM), pl.BlockSpec(memory_space=pltpu.VMEM)
    return pl.pallas_call(
        kernel,
        out_shape=[jax.ShapeDtypeStruct(shape, kind) for shape, kind in outs],
        in_specs=[smem] * len(scalars) + [vmem] * len(arrays),
        out_specs=[vmem] * len(outs),
        compiler_params=pltpu.CompilerParams(vmem_limit_bytes=limit),
    )(*scalars, *arrays)


def padded(array, dim):
    extra = -array.shape[dim] % 128
    widths = [(0, extra if d == dim else 0) for d in range(array.ndim)]
    return jnp.pad(array, widths)


def column_peaks(values):
    return jnp.max(jnp.abs(values), axis=0, keepdims=True)


def everyones(values):
    copies = jnp.broadcast_to(values, (NY * NC * NZ * NX, 1, values.shape[0]))
    return lax.all_to_all(copies, ALL, 0, 0, tiled=True).max(axis=(0, 1))


def rotate_split(matrix, block_size, wide, rows):
    total = 0.0
    for _ in range(3):
        term = lax.reduce_precision(matrix, 8, 7)
        part = term.astype(bf16)
        total = total + (dot(wide, part, 1, 0) if rows else dot(part, wide, 1, 0))
        matrix = matrix - term
    return total * block_size ** (-0.5)


def layer(tokens, cotangent, gate_weight, up_weight, down_weight):
    hid = gate_weight.shape[1]
    rows, features = tokens.shape
    core = lax.axis_index("c")
    first = core == 0

    column = copied(jnp.concatenate([tokens, cotangent], axis=0), "z", NZ)
    token_column = column[:, :rows].reshape(NZ * rows, features)
    cot_column = column[:, rows:].reshape(NZ * rows, features)

    ids = lax.optimization_barrier(jnp.arange(features, dtype=jnp.int32))
    rot_wide, hid_wide = lax.optimization_barrier(
        (wide_table(ROT_BLOCK, ids), wide_table(HID_BLOCK, ids))
    )
    pair_rot = rotate_cols(
        jnp.concatenate([padded(gate_weight.T, 0), padded(up_weight.T, 0)], axis=0),
        ROT_BLOCK,
        rot_wide,
    )
    wide = pair_rot.shape[0] // 2
    down_rot = rotate_rows(padded(down_weight, 0), HID_BLOCK, hid_wide)
    token_rot = rotate_cols(tokens, ROT_BLOCK, rot_wide)
    tops = jnp.concatenate(
        [
            column_peaks(pair_rot[:wide]),
            column_peaks(pair_rot[wide:]),
            column_peaks(down_rot),
            column_peaks(token_rot),
        ],
        axis=0,
    )
    peaks = everyones(after(tops.max(axis=1), column))
    in_scales = peaks[:2] / fp_top
    small_table = after(hid_wide[:128, :128], column)
    gate_peak, up_peak, down_peak, token_peak = (peaks[k : k + 1, None] for k in range(4))
    pair_peak = jnp.where(jnp.arange(2 * wide)[:, None] < wide, gate_peak, up_peak)
    weight_pair = soft_cast(pair_rot, pair_peak)
    down_cast = soft_cast(down_rot, down_peak)

    mine_tokens, their_tokens = halves_along_x(blocks_along_x(token_column), first)
    cot_blocks = blocks_along_x(cot_column)

    their_tok = soft_cast(rotate_cols(their_tokens, ROT_BLOCK, rot_wide), token_peak)
    mine_tok = soft_cast(rotate_cols(mine_tokens, ROT_BLOCK, rot_wide), token_peak)

    their_pair = (dot(their_tok, weight_pair, 1, 1) * 2.0**-12).astype(f16)
    mine_pair = dot(mine_tok, weight_pair, 1, 1) * 2.0**-12
    pair_blocks = sum_with_other_core(mine_pair, their_pair)
    pair_sums, pair_sends = scatter_width(pair_blocks, f16)
    mine_cot, their_cot = halves_along_x(after(cot_blocks, pair_sends), first)
    their_back = (dot(their_cot, down_cast, 1, 1) * 2.0**-6).astype(f16)
    mine_back = dot(mine_cot, down_cast, 1, 1) * 2.0**-6
    back_blocks = sum_with_other_core(mine_back, their_back)
    back_sums, _ = scatter_width(back_blocks, f16)
    scales = jnp.concatenate(
        [
            token_peak * gate_peak / (fp_top * fp_top) * 2.0**12,
            token_peak * up_peak / (fp_top * fp_top) * 2.0**12,
            down_peak / fp_top * 2.0**6,
        ],
        axis=0,
    )
    acts, hidden_top = call(
        middle_kernel,
        [((pair_sums.shape[0], 3 * wide), bf16), ((8, 128), f32)],
        [],
        [pair_sums, back_sums, jnp.broadcast_to(scales, (3, wide)), small_table],
    )
    mine_acts, their_acts = gather_half(acts)

    hidden_tops = copied(hidden_top.max(axis=0, keepdims=True), ALL, NY * NC * NZ * NX)

    quarter = mine_acts.shape[0] // 2
    part, piece = ((quarter, features), f32), ((quarter, features), bf16)
    in_mine, near = call(in_mine_kernel, [part, piece], [in_scales], [mine_acts, weight_pair])
    keep, far, last = call(
        in_their_kernel,
        [part, piece, piece],
        [core[None], in_scales],
        [their_acts, weight_pair, in_mine],
    )
    in_column = sum_along_x(keep, far, near, last)

    hidden_tops = after(hidden_tops, keep, far, last).reshape(-1, 128)
    cast = ((2 * quarter, wide), bf16)
    out_mine, near, mine_hid_cast, hidden_peak = call(
        out_mine_kernel,
        [part, piece, cast, ((8, features), f32)],
        [],
        [hidden_tops, mine_acts, small_table, down_cast],
    )
    keep, far, last, their_hid_cast = call(
        out_their_kernel,
        [part, piece, piece, cast],
        [core[None]],
        [hidden_tops, their_acts, small_table, down_cast, out_mine],
    )
    out_column = sum_along_x(keep, far, near, last)
    hidden_peak = hidden_peak[:1]

    in_arrived = pieces_along_z(in_column)
    input_sum = in_arrived.astype(f32).sum(axis=0)
    input_grad = rotate_cols(input_sum, ROT_BLOCK).astype(bf16)
    out_arrived = pieces_along_z(after(out_column, in_arrived))
    out_sum = out_arrived.astype(f32).sum(axis=0)
    output = (out_sum * (hidden_peak * down_peak / (fp_top * fp_top))).astype(bf16)

    mine_hid_cast, their_hid_cast = after((mine_hid_cast, their_hid_cast), keep)
    down_dot = dot(mine_hid_cast, mine_cot, 0, 0) + dot(their_hid_cast, their_cot, 0, 0)
    down_grad = rotate_split(down_dot, HID_BLOCK, hid_wide, True) * (hidden_peak / fp_top)
    down_grad = down_grad[:hid].astype(bf16)
    mine_tok, their_tok = after((mine_tok, their_tok), keep, in_column)
    pair_dot = dot(mine_acts[:, : 2 * wide], mine_tok, 0, 0) + dot(
        their_acts[:, : 2 * wide], their_tok, 0, 0
    )
    pair_grad = rotate_split(pair_dot * (token_peak / fp_top), ROT_BLOCK, rot_wide, False)
    pair_grad = pair_grad.astype(bf16)
    return (
        output,
        input_grad,
        pair_grad[:hid].T,
        pair_grad[wide : wide + hid].T,
        down_grad,
    )


def solution(mesh):
    split = Mesh(mesh.devices.reshape(NY, NC, NZ, NX), ALL)
    placed = (P(GY, GX), P(GY, GX), P(GX, GY), P(GX, GY), P(GY, GX))
    return jax.shard_map(
        layer,
        mesh=split,
        in_specs=placed,
        out_specs=(P(GY, GX), P(GY, GX), P(GX, GY), P(GX, GY), P(GY, GX)),
        check_vma=False,
    )
```
